32 devices in a mesh: dp: 8 (over z, x), mp: 4 (over y, core).
Axes of the slice: x: 2, y: 2, z: 4, core: 2. Of those that a mesh axis runs over, the one named last changes fastest.
Arguments:
- gradients: bfloat16 [8, 2, 4096, 1024], P('dp', None, None, 'mp'), may hold values from -6912 to 6912
- layer_mask: int32 [8, 2], P('dp'), may hold values from 0 to 1, as said below
- exit_losses: float32 [8, 2], P('dp'), may hold values from 1 to 24
- exit_weights: int32 [2], replicated, may hold values from 1 to 8
- params: float32 [2, 4096, 1024], P(None, 'dp', 'mp'), may hold values from -0.3 to 0.3
- moment: float32 [2, 4096, 1024], P(None, 'dp', 'mp'), may hold values from -6 to 6
- second: float32 [2, 4096, 1024], P(None, 'dp', 'mp'), may hold values from 0.5 to 4
Outputs:
- new_params: float32 [2, 4096, 1024], P(None, 'dp', 'mp')
- new_moment: float32 [2, 4096, 1024], P(None, 'dp', 'mp')
- new_second: float32 [2, 4096, 1024], P(None, 'dp', 'mp')
- exit_mean: float32 [2], replicated
The draws below stay inside these ranges and needn't reach their ends.
Inputs may be any that keep to these rules, and one draw needn't show every extreme that they name: `layer_mask`: every layer is run by at least one micro-batch.
All inputs are finite; a program needn't handle non-finite values.
Results may differ from the reference program's by a relative error of at most 0.0003.
Values sent between devices are 32-bit elements; how exact they have to be, the bound alone decides.
No kernel may reach another device: no remote copies, remote signals or barrier semaphores. Data moves between devices by JAX's collectives and lax.ppermute only.
A program may use at most 64 MiB of HBM per device.

```python
import math
import jax
import jax.numpy as jnp
from jax import lax

D = 4096
KVW = 1024
LAYERS = 2
MB = 8


def draw_gradients(key, part):
    key_rows = jax.random.fold_in(key, 0)
    key_cols = jax.random.fold_in(key, 1)
    key_noise = jax.random.fold_in(key, 3)
    row_scale = jnp.exp(jax.random.uniform(key_rows, (D,), jnp.float32, math.log(0.3), math.log(3.0)))
    col_scale = jnp.exp(jax.random.uniform(key_cols, (KVW,), jnp.float32, math.log(0.3), math.log(3.0)))
    values = jax.random.normal(key_noise, (MB, LAYERS, D, KVW), jnp.float32)
    values = jnp.clip(values, -6.0, 6.0) * 128.0 * row_scale[:, None] * col_scale[None, :]
    return values.astype(jnp.bfloat16)


def draw_layer_mask(key, part):
    key_keep, key_force = jax.random.split(key)
    raw_draws = jax.random.randint(key_keep, (MB, LAYERS), 0, 1000)
    depth_index = jnp.arange(LAYERS, dtype=jnp.int32)
    threshold = 900 - 400 * depth_index // max(LAYERS - 1, 1)
    keep_flag = (raw_draws < threshold[None, :]).astype(jnp.int32)
    forced = jax.random.randint(key_force, (LAYERS,), 0, MB)
    row_index = jnp.arange(MB, dtype=jnp.int32)
    chosen = (row_index[:, None] == forced[None, :]).astype(jnp.int32)
    return jnp.maximum(keep_flag, chosen)


def draw_exit_losses(key, part):
    ramp = 1.0 + 2.0 * jnp.arange(MB, dtype=jnp.float32) / max(MB - 1, 1)
    base = jnp.exp(jax.random.uniform(key, (MB, LAYERS), jnp.float32, math.log(1.5), math.log(4.0)))
    return (ramp[:, None] * base).astype(jnp.float32)


def steps_of(stream_key, dims, cuts, smallest, high):
    level = 1.0
    for position, shards_of in cuts:
        heights = jax.random.uniform(jax.random.fold_in(jax.random.fold_in(stream_key, 6), position), (shards_of,), jnp.float32, smallest / len(cuts), high / len(cuts))
        level = level * jnp.repeat(jnp.exp(heights), dims[position] // shards_of).reshape((-1,) + (1,) * (len(dims) - 1 - position))
    return level


def gaussian(key, extent, scale, reach, shards=(), held_as=jnp.bfloat16):
    entries = scale * jax.random.normal(key, extent, jnp.float32)
    if shards:
        entries = entries * steps_of(key, extent, shards, -0.22, 0.18)
    return jnp.clip(entries, -reach, reach).astype(held_as)


def setup_inputs(seed: int = 0) -> dict:
    keys = jax.random.split(jax.random.key(seed), 8)
    gradients = draw_gradients(jax.random.fold_in(keys[7], 71), 0)
    layer_mask = draw_layer_mask(jax.random.fold_in(keys[7], 71), 0)
    exit_losses = draw_exit_losses(jax.random.fold_in(keys[7], 71), 0)
    exit_weights = jax.random.randint(keys[3], (LAYERS,), 1, 9).astype(jnp.int32)
    params = gaussian(keys[4], (LAYERS, D, KVW), 0.05, 0.3, ((1, 8), (2, 4)), jnp.float32)
    moment = gaussian(keys[5], (LAYERS, D, KVW), 1.0, 6.0, ((1, 8), (2, 4)), jnp.float32)
    second = jnp.clip(jnp.exp(math.log(4.0) - 2.0794415 * jax.random.uniform(keys[6], (LAYERS, D, KVW), jnp.float32) ** steps_of(keys[6], (LAYERS, D, KVW), ((1, 8), (2, 4)), -0.2, 0.2)), 0.5, 4.0)
    return dict(gradients=gradients, layer_mask=layer_mask, exit_losses=exit_losses, exit_weights=exit_weights, params=params, moment=moment, second=second)


max_rms = 1.0
eps_norm = 1e-06
eps_adam = 1e-08
beta_one = 0.9
beta_two = 0.95
learn_rate = 0.01
decay_rate = 0.1

def reference(gradients, layer_mask, exit_losses, exit_weights, params, moment, second):
    keep_float = layer_mask.astype(jnp.float32)
    layer_count = lax.optimization_barrier(jnp.sum(keep_float, axis=0))
    exit_mean = lax.optimization_barrier(jnp.sum(keep_float * exit_losses, axis=0)) / layer_count
    weight_float = exit_weights.astype(jnp.float32)
    weight_sum = jnp.sum(weight_float)

    def accumulate(running, pieces):
        block, keep_row = pieces
        return (running + block.astype(jnp.float32) * keep_row[:, None, None], None)
    summed, unused = lax.scan(accumulate, jnp.zeros((LAYERS, D, KVW), jnp.float32), (gradients, keep_float))
    factor_row = weight_float / (weight_sum * layer_count)
    gradient = summed * factor_row[:, None, None]
    rms_value = jnp.sqrt(jnp.sum(gradient * gradient) / (LAYERS * D * KVW))
    clip_scale = jnp.minimum(1.0, max_rms / (rms_value + eps_norm))
    clipped = clip_scale * gradient
    new_moment = beta_one * moment + (1.0 - beta_one) * clipped
    new_second = beta_two * second + (1.0 - beta_two) * clipped * clipped
    new_params = params - learn_rate * (new_moment / (jnp.sqrt(new_second) + eps_adam) + decay_rate * params)
    return (new_params, new_moment, new_second, exit_mean)
```

```python
import jax
import jax.numpy as jnp
from jax import lax
from jax.experimental import pallas as pl
from jax.experimental.pallas import tpu as pltpu
from jax.sharding import PartitionSpec as P

max_rms = 1.0
eps_norm = 1e-06
eps_adam = 1e-08
beta_one = 0.9
beta_two = 0.95
learn_rate = 0.01
decay_rate = 0.1


ROW_TILE = 16


def widen_kernel(shard_ref, keep_ref, grad_ref, out_ref):
    scale = keep_ref[pl.program_id(0)]
    out_ref[0] = grad_ref[0, 0].astype(jnp.float32) * scale


def widen(shard, keep, grad, rows):
    layers, n, pair, full, cols = grad.shape
    source = grad.reshape(layers, n * pair, full, cols)
    size = layers * rows * cols
    return pl.pallas_call(
        widen_kernel,
        grid_spec=pltpu.PrefetchScalarGridSpec(
            num_scalar_prefetch=2,
            grid=(layers,),
            in_specs=[
                pl.BlockSpec((1, 1, rows, cols), lambda layer, shard, keep: (layer, shard[0], 0, 0))
            ],
            out_specs=pl.BlockSpec((1, rows, cols), lambda layer, shard, keep: (layer, 0, 0)),
        ),
        out_shape=jax.ShapeDtypeStruct((layers, rows, cols), jnp.float32),
        cost_estimate=pl.CostEstimate(flops=size, bytes_accessed=6 * size, transcendentals=0),
        name="widen",
    )(shard.reshape(1), keep, source)


def make_body(n_dp, n_mp):
    pair = 2 if n_dp % 2 == 0 else 1
    n = n_dp // pair

    def swap():
        return [(i, i ^ 1) for i in range(n_dp)]

    def up(j):
        return [(z * pair + x, (z + 1) * pair + x) for z in range(j + 1) for x in range(pair)]

    def down(j):
        return [
            ((n - 1 - z) * pair + x, (n - 2 - z) * pair + x)
            for z in range(j + 1)
            for x in range(pair)
        ]

    def order(z, k):
        def lower(z, k):
            if k == n - 1:
                return z
            return jnp.where(k < z, k, n - 1 - k + z)

        mirrored = n - 1 - lower(n - 1 - z, k)
        return jnp.clip(jnp.where(2 * z < n, lower(z, k), mirrored), 0, n - 1)

    def body(gradients, layer_mask, exit_losses, exit_weights, params, moment, second):
        layers, width, cols = gradients.shape[1:]
        rows = width // n_dp
        index = lax.axis_index("dp")
        z, x = index // pair, index % pair
        keep = layer_mask[0].astype(jnp.float32)
        grad = gradients[0].reshape(layers, n, pair, rows, cols)

        rows_b = 0
        use_b = False
        if use_b and pair == 2 and n > 1:
            rows_b = round(rows / (2 * (n - 1)) / ROW_TILE) * ROW_TILE
        rows_a = rows - rows_b

        def local_a(shard, side):
            got = lax.dynamic_index_in_dim(grad, shard, 1, keepdims=False)
            got = lax.dynamic_index_in_dim(got, side, 1, keepdims=False)
            return got[:, :rows_a].astype(jnp.float32) * keep[:, None, None]

        def local_b(shard):
            got = lax.dynamic_index_in_dim(grad, shard, 1, keepdims=False)
            return got[:, :, rows_a:].astype(jnp.float32) * keep[:, None, None, None]

        def up_shard(j):
            return jnp.clip(n - 1 - j + z, 0, n - 1)

        def down_shard(j):
            return jnp.clip(j - (n - 1) + z, 0, n - 1)

        pieces = []
        if pair == 2:
            for k in range(n):
                part = widen(order(z, k) * pair + 1 - x, keep, grad, rows_a)
                pieces.append(lax.ppermute(part, "dp", swap()))

        b_up = b_dn = None
        if rows_b:
            for j in range(n - 1):
                send = local_b(up_shard(j))
                if j:
                    send = send + b_up
                b_up = lax.ppermute(send, "dp", up(j))
                send = local_b(down_shard(j))
                if j:
                    send = send + b_dn
                b_dn = lax.ppermute(send, "dp", down(j))
            total = local_b(z) + b_up + b_dn
            away = lax.dynamic_index_in_dim(total, 1 - x, 1, keepdims=False)
            stay = lax.dynamic_index_in_dim(total, x, 1, keepdims=False)
            sum_b = stay + lax.ppermute(away, "dp", swap())

        def piece(j, place):
            got = pieces[j]
            for far in range((n + 1) // 2, j + 1):
                got = jnp.where(place == far, pieces[j - far], got)
            return got

        a_up = a_dn = None
        for j in range(n - 1):
            send = local_a(up_shard(j), x)
            if pieces:
                send = send + piece(j, z)
            if j:
                send = send + a_up
            a_up = lax.ppermute(send, "dp", up(j))
            send = local_a(down_shard(j), x)
            if pieces:
                send = send + piece(j, n - 1 - z)
            if j:
                send = send + a_dn
            a_dn = lax.ppermute(send, "dp", down(j))
        sum_a = local_a(z, x)
        if pieces:
            sum_a = sum_a + pieces[n - 1]
        if n > 1:
            sum_a = sum_a + a_up + a_dn

        squares = jnp.sum(sum_a * sum_a, axis=(1, 2))
        if rows_b:
            squares = squares + jnp.sum(sum_b * sum_b, axis=(1, 2))
            summed = jnp.concatenate([sum_a, sum_b], axis=1)
        else:
            summed = sum_a

        first = (lax.axis_index("mp") == 0).astype(jnp.float32)
        stats = jnp.stack([squares, first * keep, first * keep * exit_losses[0]])
        every = n_dp * n_mp
        sent = jnp.broadcast_to(stats.reshape(1, -1), (every, stats.size))
        stats = jnp.sum(lax.all_to_all(sent, ("dp", "mp"), 0, 0), axis=0).reshape(stats.shape)
        squares, layer_count, loss_sum = stats[0], stats[1], stats[2]

        weight_float = exit_weights.astype(jnp.float32)
        factor = weight_float / (jnp.sum(weight_float) * layer_count)
        exit_mean = loss_sum / layer_count
        square_sum = jnp.sum(factor * factor * squares)
        rms_value = jnp.sqrt(square_sum / (layers * width * cols * n_mp))
        clip_scale = jnp.minimum(1.0, max_rms / (rms_value + eps_norm))
        clipped = (clip_scale * factor)[:, None, None] * summed
        new_moment = beta_one * moment + (1.0 - beta_one) * clipped
        new_second = beta_two * second + (1.0 - beta_two) * clipped * clipped
        new_params = params - learn_rate * (
            new_moment / (jnp.sqrt(new_second) + eps_adam) + decay_rate * params
        )
        return (new_params, new_moment, new_second, exit_mean)

    return body


def solution(mesh):
    placed = (
        P("dp", None, None, "mp"),
        P("dp", None),
        P("dp", None),
        P(),
        P(None, "dp", "mp"),
        P(None, "dp", "mp"),
        P(None, "dp", "mp"),
    )
    return jax.shard_map(
        make_body(mesh.shape["dp"], mesh.shape["mp"]),
        mesh=mesh,
        in_specs=placed,
        out_specs=(P(None, "dp", "mp"), P(None, "dp", "mp"), P(None, "dp", "mp"), P()),
        check_vma=False,
    )
```
